8 devices in a mesh: stage: 2 (over z, y), data: 4 (over x, core).
Axes of the slice: x: 2, y: 2, z: 1, core: 2. Of those that a mesh axis runs over, the one named last changes fastest.
Arguments:
- w_master: float32 [64, 2048, 768], P('stage', 'data'), parts along dimension 0
- momentum: float32 [64, 2048, 768], P('stage', 'data'), parts along dimension 0
- grad: bfloat16 [64, 2048, 768], P('stage', 'data'), parts along dimension 0
Outputs:
- output 1: bfloat16 [64, 2048, 768], P('stage'), parts along dimension 0
- output 2: float32 [64, 2048, 768], P('stage', 'data'), parts along dimension 0
There are 2 independent parts. The reference program is written for one: setup_inputs(seed, part) draws one part's arguments, and reference() takes and returns one part's arrays. A program takes and returns all parts, laid end to end along the dimension named above; each array names one.
All inputs are finite; a program needn't handle non-finite values.
Results may differ from the reference program's by a relative error of at most 0.00720861.
Values are sent between devices in bfloat16 or wider.
A program may use at most 1.25 GiB of HBM per device.

```python
import math
import jax
import jax.numpy as jnp
from jax import lax

DATA_DEVS = 4
MATS_DEV = 8
D = 2048
FF_E = 768
NS_ITERS = 5

MOMENTUM = 0.95
LEARN_RATE = 0.02
WEIGHT_DECAY = 0.1
NORM_EPS = 1e-7
COEF_A = 3.4445
COEF_B = -4.7750
COEF_C = 2.0315
RMS_SCALE = 0.2 * math.sqrt(max(D, FF_E))


def setup_inputs(seed: int = 0, part: int = 0) -> dict:
    mat_count = MATS_DEV * DATA_DEVS
    key = jax.random.fold_in(jax.random.key(seed), part)
    keys = jax.random.split(key, 7)
    w_master = 0.02 * jax.random.normal(keys[0], (mat_count, D, FF_E), jnp.float32)
    left_fac = jax.random.normal(keys[1], (mat_count, D, 4), jnp.float32)
    right_fac = jax.random.normal(keys[2], (mat_count, 4, FF_E), jnp.float32)
    shared = 0.25 * jnp.einsum("mdr,mrf->mdf", left_fac, right_fac)
    row_scale = jax.random.uniform(keys[3], (mat_count, D, 1), jnp.float32, 0.5, 2.0)
    momentum = row_scale * (jax.random.normal(keys[4], (mat_count, D, FF_E), jnp.float32) + shared)
    grad_scale = jax.random.uniform(keys[5], (mat_count, D, 1), jnp.float32, 0.5, 2.0)
    grad = (grad_scale * jax.random.normal(keys[6], (mat_count, D, FF_E), jnp.float32)).astype(jnp.bfloat16)
    return {"w_master": w_master, "momentum": momentum, "grad": grad}


def newton_schulz(x_mat):
    for iteration in range(NS_ITERS):
        gram_mat = jnp.dot(x_mat, x_mat.T, preferred_element_type=jnp.float32).astype(jnp.bfloat16)
        square = jnp.dot(gram_mat, gram_mat, preferred_element_type=jnp.float32)
        poly_mat = (COEF_B * gram_mat.astype(jnp.float32) + COEF_C * square).astype(jnp.bfloat16)
        prod_mat = jnp.dot(poly_mat, x_mat, preferred_element_type=jnp.float32)
        x_mat = (COEF_A * x_mat.astype(jnp.float32) + prod_mat).astype(jnp.bfloat16)
    return x_mat


def orthogonalize(mom_one):
    frob_norm = jnp.sqrt(jnp.sum(mom_one * mom_one))
    x_mat = (mom_one.astype(jnp.bfloat16).astype(jnp.float32) / (frob_norm + NORM_EPS)).astype(jnp.bfloat16)
    if D > FF_E:
        x_mat = newton_schulz(x_mat.T).T
    else:
        x_mat = newton_schulz(x_mat)
    return x_mat.astype(jnp.float32) * RMS_SCALE


def reference(w_master, momentum, grad):
    mom_new = MOMENTUM * momentum + grad.astype(jnp.float32)

    def update_one(w_and_m):
        w_one, mom_one = w_and_m
        w_new = w_one - LEARN_RATE * (orthogonalize(mom_one) + WEIGHT_DECAY * w_one)
        return w_new.astype(jnp.bfloat16)

    params = lax.map(update_one, (w_master, mom_new))
    return params, mom_new
```

```python
import functools
import math

import jax
import jax.numpy as jnp
from jax import lax
from jax.experimental import pallas as pl
from jax.experimental.pallas import tpu as pltpu
from jax.sharding import PartitionSpec as P


NS_ITERS = 5
MOMENTUM = 0.95
LEARN_RATE = 0.02
WEIGHT_DECAY = 0.1
NORM_EPS = 1e-7
COEF_A = 3.4445
COEF_B = -4.7750
COEF_C = 2.0315

GROUP = 4
CHUNKS = (1, 7, 8, 8, 4, 2, 1, 1)
FIRSTS = tuple(sum(CHUNKS[:c]) for c in range(len(CHUNKS)))
ORDER = (2, 3, 1, 0)
X_PERM = ((0, 2), (1, 3), (2, 0), (3, 1))
CORE_PERM = ((0, 1), (1, 0), (2, 3), (3, 2))


def relations(me):
    partner = me + 1 - 2 * lax.rem(me, 2)
    return me, partner, lax.rem(me + 2, GROUP), lax.rem(partner + 2, GROUP)


def exchange_kernel(rounds, rms_scale, w_ref, mom_ref, grad_ref, *refs):
    n = len(CHUNKS)
    w_outs, (w_chip, mb, xin, oo, orv) = refs[:n], refs[n : n + 5]
    (fbuf, hbuf, sbuf, ss_loc, ss_in, xa, xb, amat, bmat, f_sem, h_sem, st_sem, x_sem,
     m_send, m_recv, s_send, s_recv, o_send, o_recv, w_send, w_recv) = refs[n + 5 :]
    rows, cols = mom_ref.shape[1], mom_ref.shape[2]
    rel = relations(lax.axis_index("data"))
    strip = 64

    barrier = pltpu.get_barrier_semaphore()
    for k in (1, 2, 3):
        pl.semaphore_signal(barrier, inc=1, device_id={"data": rel[k]}, device_id_type=pl.DeviceIdType.MESH)
    pl.semaphore_wait(barrier, GROUP - 1)

    def remote(src, dst, send, recv, k):
        return pltpu.make_async_remote_copy(
            src_ref=src, dst_ref=dst, send_sem=send, recv_sem=recv,
            device_id={"data": rel[k]}, device_id_type=pl.DeviceIdType.MESH)

    def load_m(r, k, slot):
        m = GROUP * r + rel[k]
        return (pltpu.make_async_copy(mom_ref.at[m], fbuf.at[slot], f_sem.at[slot]),
                pltpu.make_async_copy(grad_ref.at[m], hbuf.at[slot], h_sem.at[slot]))

    def stage_m(r, k, slot):
        dst = xin.at[r, pl.ds(0, rows)] if k == 0 else mb.at[r, k - 1]
        return pltpu.make_async_copy(sbuf.at[slot], dst, st_sem.at[slot])

    def send_m(r, k):
        return (remote(mb.at[r, k - 1], xin.at[r, pl.ds(k * rows, rows)], m_send.at[r, k - 1], m_recv.at[r, k - 1], k),
                remote(ss_loc.at[r, k - 1], ss_in.at[r, k], s_send.at[r, k - 1], s_recv.at[r, k - 1], k))

    for copy in load_m(0, ORDER[0], 0):
        copy.start()

    def momentum_round(r, carry):
        for j, k in enumerate(ORDER):
            slot = j % 2
            for copy in load_m(r, k, slot):
                copy.wait()
            if j + 1 < GROUP:
                for copy in load_m(r, ORDER[j + 1], 1 - slot):
                    copy.start()
            else:
                @pl.when(r + 1 < rounds)
                def _():
                    for copy in load_m(r + 1, ORDER[0], 1 - slot):
                        copy.start()

            def part(i, acc):
                sl = pl.ds(pl.multiple_of(i * strip, strip), strip)
                mom_new = MOMENTUM * fbuf[slot, sl, :] + hbuf[slot, sl, :].astype(jnp.float32)
                sbuf[slot, sl, :] = mom_new.astype(jnp.bfloat16)
                return acc + jnp.sum((mom_new * mom_new).reshape(strip // 8, 8, cols), axis=0)

            acc = lax.fori_loop(0, rows // strip, part, jnp.zeros((8, cols), jnp.float32))
            total = jnp.broadcast_to(jnp.sum(jnp.sum(acc, axis=0, keepdims=True), axis=1, keepdims=True), (8, 128))
            if k == 0:
                ss_in[r, 0] = total
            else:
                ss_loc[r, k - 1] = total
            stage_m(r, k, slot).start()
            if j > 0:
                before = ORDER[j - 1]
                stage_m(r, before, 1 - slot).wait()
                for copy in send_m(r, before):
                    copy.start()
            else:
                @pl.when(r > 0)
                def _():
                    stage_m(r - 1, ORDER[-1], 1 - slot).wait()
        return carry

    lax.fori_loop(0, rounds, momentum_round, 0)
    stage_m(rounds - 1, ORDER[-1], (GROUP - 1) % 2).wait()

    def send_o(r, k):
        return remote(oo.at[r, pl.ds(k * rows, rows)], orv.at[r, rel[0]], o_send.at[r, k - 1], o_recv.at[r, k - 1], k)

    def ortho_round(r, carry):
        for k in (1, 2, 3):
            for copy in send_m(r, k):
                copy.wait_recv()
        fetch = pltpu.make_async_copy(xin.at[r], xa, x_sem)
        fetch.start()
        fetch.wait()
        total = ss_in[r, 0] + ss_in[r, 1] + ss_in[r, 2] + ss_in[r, 3]
        denom = (jnp.sqrt(total) + NORM_EPS)[0:1, 0:1]

        def scale(i, c):
            sl = pl.ds(pl.multiple_of(i * strip, strip), strip)
            xb[sl, :] = (xa[sl, :].astype(jnp.float32) / denom).astype(jnp.bfloat16)
            return c

        lax.fori_loop(0, GROUP * rows // strip, scale, 0)

        def iterate(_, c):
            x_mat = xb[...]
            amat[...] = lax.dot_general(x_mat, x_mat, (((0,), (0,)), ((), ())),
                                        preferred_element_type=jnp.float32).astype(jnp.bfloat16)
            a_mat = amat[...]
            square = jnp.dot(a_mat, a_mat, preferred_element_type=jnp.float32)
            bmat[...] = (COEF_B * a_mat.astype(jnp.float32) + COEF_C * square).astype(jnp.bfloat16)

            def update(i, c2):
                sl = pl.ds(pl.multiple_of(i * rows, rows), rows)
                x_rows = xb[sl, :]
                prod = jnp.dot(x_rows, bmat[...], preferred_element_type=jnp.float32)
                xb[sl, :] = (COEF_A * x_rows.astype(jnp.float32) + prod).astype(jnp.bfloat16)
                return c2

            return lax.fori_loop(0, GROUP, update, c)

        lax.fori_loop(0, NS_ITERS, iterate, 0)
        kept = pltpu.make_async_copy(xb.at[pl.ds(0, rows)], orv.at[r, rel[0]], f_sem.at[0])
        out = pltpu.make_async_copy(xb, oo.at[r], x_sem)
        out.start()
        kept.start()
        out.wait()
        for k in ORDER[:3]:
            send_o(r, k).start()
        kept.wait()
        return carry

    lax.fori_loop(0, rounds, ortho_round, 0)

    def load_w(m, slot):
        return (pltpu.make_async_copy(w_ref.at[m], fbuf.at[slot], f_sem.at[slot]),
                pltpu.make_async_copy(orv.at[m // GROUP, lax.rem(m, GROUP)], hbuf.at[slot], h_sem.at[slot]))

    def load_round(m, slot):
        for k in (1, 2, 3):
            send_o(m // GROUP, k).wait_recv()
        for copy in load_w(m, slot):
            copy.start()

    def stage_w(c, i, slot):
        return pltpu.make_async_copy(sbuf.at[slot], w_outs[c].at[i], st_sem.at[slot])

    def send_w(i):
        return remote(w_outs[0].at[i], w_chip.at[i], w_send.at[i], w_recv.at[i], 2)

    mats = GROUP * rounds
    load_round(0, 0)

    def weights(m, carry):
        slot, later = lax.rem(m, 2), m + 1
        for copy in load_w(m, slot):
            copy.wait()

        @pl.when(lax.rem(later, GROUP) != 0)
        def _():
            for copy in load_w(later, 1 - slot):
                copy.start()

        @pl.when(m >= 2)
        def _():
            stage_w(0, 0, slot).wait()

        @pl.when(m == CHUNKS[0] + 1)
        def _():
            for i in range(CHUNKS[0]):
                send_w(i).start()

        def part(i, c):
            sl = pl.ds(pl.multiple_of(i * strip, strip), strip)
            w_old = fbuf[slot, sl, :]
            ortho = hbuf[slot, sl, :].astype(jnp.float32) * rms_scale
            sbuf[slot, sl, :] = (w_old - LEARN_RATE * (ortho + WEIGHT_DECAY * w_old)).astype(jnp.bfloat16)
            return c

        lax.fori_loop(0, rows // strip, part, 0)
        for c in range(n):
            @pl.when((m >= FIRSTS[c]) & (m < FIRSTS[c] + CHUNKS[c]))
            def _():
                stage_w(c, m - FIRSTS[c], slot).start()

        @pl.when((lax.rem(later, GROUP) == 0) & (later < mats))
        def _():
            load_round(later, 1 - slot)

        return carry

    lax.fori_loop(0, mats, weights, 0)
    stage_w(0, 0, 0).wait()
    stage_w(0, 0, 1).wait()
    for i in range(CHUNKS[0]):
        send_w(i).wait()

    def drain(r, carry):
        for k in (1, 2, 3):
            for copy in send_m(r, k):
                copy.wait_send()
            send_o(r, k).wait_send()
        return carry

    lax.fori_loop(0, rounds, drain, 0)


def exchange(w_rows, mom_rows, grad_rows):
    mats, rows, cols = mom_rows.shape
    rounds = mats // GROUP
    half, full = jnp.bfloat16, jnp.float32
    rms_scale = 0.2 * math.sqrt(max(rows * GROUP, cols))
    shapes = [jax.ShapeDtypeStruct((count, rows, cols), half) for count in CHUNKS + CHUNKS[:1]] + [
        jax.ShapeDtypeStruct((rounds, 3, rows, cols), half),
        jax.ShapeDtypeStruct((rounds, GROUP * rows, cols), half),
        jax.ShapeDtypeStruct((rounds, GROUP * rows, cols), half),
        jax.ShapeDtypeStruct((rounds, GROUP, rows, cols), half),
    ]
    dma = pltpu.SemaphoreType.DMA
    flops = rounds * NS_ITERS * 2 * cols * cols * (2 * rows * GROUP + cols)
    outs = pl.pallas_call(
        functools.partial(exchange_kernel, rounds, rms_scale),
        out_shape=shapes,
        in_specs=[pl.BlockSpec(memory_space=pltpu.HBM)] * 3,
        out_specs=[pl.BlockSpec(memory_space=pltpu.HBM)] * len(shapes),
        scratch_shapes=[
            pltpu.VMEM((2, rows, cols), full),
            pltpu.VMEM((2, rows, cols), half),
            pltpu.VMEM((2, rows, cols), half),
            pltpu.VMEM((rounds, 3, 8, 128), full),
            pltpu.VMEM((rounds, GROUP, 8, 128), full),
            pltpu.VMEM((GROUP * rows, cols), half),
            pltpu.VMEM((GROUP * rows, cols), half),
            pltpu.VMEM((cols, cols), half),
            pltpu.VMEM((cols, cols), half),
            dma((2,)), dma((2,)), dma((2,)), dma,
            *[dma((rounds, 3))] * 6, *[dma((CHUNKS[0],))] * 2,
        ],
        compiler_params=pltpu.CompilerParams(collective_id=0, has_side_effects=True, vmem_limit_bytes=60 * 1024 * 1024),
        cost_estimate=pl.CostEstimate(flops=flops, bytes_accessed=12 * mats * rows * cols, transcendentals=0),
        name="exchange",
    )(w_rows, mom_rows, grad_rows)
    return outs[: len(CHUNKS)], outs[len(CHUNKS)]


def place_kernel(first, parts, *refs):
    blocks, (out_ref, buf, in_sem, out_sem) = refs[: len(parts)], refs[-4:]
    count, rows, _ = blocks[0].shape
    rel = relations(lax.axis_index("data"))

    def fetch(i, n, slot):
        return pltpu.make_async_copy(blocks[n].at[i], buf.at[slot, n], in_sem.at[slot, n])

    def put(i, n, slot):
        dst = out_ref.at[first + i, pl.ds(pl.multiple_of(rel[parts[n]] * rows, rows), rows)]
        return pltpu.make_async_copy(buf.at[slot, n], dst, out_sem.at[slot, n])

    for n in range(len(parts)):
        fetch(0, n, 0).start()

    def step(i, carry):
        slot = lax.rem(i, 2)
        for n in range(len(parts)):
            @pl.when(i >= 1)
            def _():
                put(i - 1, n, 1 - slot).wait()

            @pl.when(i + 1 < count)
            def _():
                fetch(i + 1, n, 1 - slot).start()

        for n in range(len(parts)):
            fetch(i, n, slot).wait()
            put(i, n, slot).start()
        return carry

    lax.fori_loop(0, count, step, 0)
    for n in range(len(parts)):
        put(count - 1, n, (count - 1) % 2).wait()


def place(chunk, blocks, dst, mats):
    parts = tuple(blocks)
    count, rows, cols = blocks[parts[0]].shape
    args, aliases = [blocks[k] for k in parts], {}
    if dst is not None:
        aliases = {len(args): 0}
        args.append(dst)
    size = len(parts) * count * rows * cols
    dma = pltpu.SemaphoreType.DMA
    return pl.pallas_call(
        functools.partial(place_kernel, FIRSTS[chunk], parts),
        out_shape=jax.ShapeDtypeStruct((mats, rows * GROUP, cols), jnp.bfloat16),
        in_specs=[pl.BlockSpec(memory_space=pltpu.HBM)] * len(args),
        out_specs=pl.BlockSpec(memory_space=pltpu.HBM),
        scratch_shapes=[pltpu.VMEM((2, len(parts), rows, cols), jnp.bfloat16), dma((2, len(parts))), dma((2, len(parts)))],
        input_output_aliases=aliases,
        cost_estimate=pl.CostEstimate(flops=size, bytes_accessed=4 * size, transcendentals=0),
        name="place",
    )(*args)


def solution(mesh):
    row_spec = P("stage", "data", None)
    full_spec = P("stage", None, None)
    last = len(CHUNKS) - 1

    def local_step(w_rows, mom_rows, grad_rows):
        mats = mom_rows.shape[0]
        own, w_chip = exchange(w_rows, mom_rows, grad_rows)
        chip, core, diag = [w_chip], [], []
        for c in range(1, last + 1):
            chip.append(lax.ppermute(own[c], "data", X_PERM))
        for c in range(last + 1):
            core.append(lax.ppermute(own[c], "data", CORE_PERM))
            diag.append(lax.ppermute(chip[c], "data", CORE_PERM))
        mom_late, grad_late, _ = lax.optimization_barrier((mom_rows, grad_rows, own[0]))
        mom_new = MOMENTUM * mom_late + grad_late.astype(jnp.float32)
        params = None
        for c in range(last):
            params = place(c, {0: own[c], 1: core[c], 2: chip[c], 3: diag[c]}, params, mats)
        params = place(last, {0: own[last], 1: core[last], 2: chip[last]}, params, mats)
        params = place(last, {3: diag[last]}, params, mats)
        return params, mom_new

    return jax.shard_map(local_step, mesh=mesh, in_specs=(row_spec, row_spec, row_spec), out_specs=(full_spec, row_spec), check_vma=False)
```

```python
import functools
import math

import jax
import jax.numpy as jnp
from jax import lax
from jax.experimental import pallas as pl
from jax.experimental.pallas import tpu as pltpu
from jax.sharding import PartitionSpec as P


NS_ITERS = 5
MOMENTUM = 0.95
LEARN_RATE = 0.02
WEIGHT_DECAY = 0.1
NORM_EPS = 1e-7
COEF_A = 3.4445
COEF_B = -4.7750
COEF_C = 2.0315

GROUP = 4
CHUNKS = (2, 6, 8, 8, 4, 2, 1, 1)
FIRSTS = tuple(sum(CHUNKS[:c]) for c in range(len(CHUNKS)))
PIECES = 4
ORDER = (2, 3, 1, 0)
X_PERM = ((0, 2), (1, 3), (2, 0), (3, 1))
CORE_PERM = ((0, 1), (1, 0), (2, 3), (3, 2))


def relations(me):
    partner = me + 1 - 2 * lax.rem(me, 2)
    return me, partner, lax.rem(me + 2, GROUP), lax.rem(partner + 2, GROUP)


def exchange_kernel(rounds, rms_scale, w_ref, mom_ref, grad_ref, *refs):
    n = len(CHUNKS)
    w_outs, (w_chip, mb, xin, oo, orv) = refs[:n], refs[n : n + 5]
    (fbuf, hbuf, sbuf, ss_loc, ss_in, xa, xb, amat, bmat, f_sem, h_sem, st_sem, x_sem,
     m_send, m_recv, s_send, s_recv, o_send, o_recv, w_send, w_recv, turn,
     pf_sem, ph_sem, ps_sem) = refs[n + 5 :]
    rows, cols = mom_ref.shape[1], mom_ref.shape[2]
    rel = relations(lax.axis_index("data"))
    strip = 64

    barrier = pltpu.get_barrier_semaphore()
    for k in (1, 2, 3):
        pl.semaphore_signal(barrier, inc=1, device_id={"data": rel[k]}, device_id_type=pl.DeviceIdType.MESH)

    def remote(src, dst, send, recv, k):
        return pltpu.make_async_remote_copy(
            src_ref=src, dst_ref=dst, send_sem=send, recv_sem=recv,
            device_id={"data": rel[k]}, device_id_type=pl.DeviceIdType.MESH)

    def load_m(r, k, slot):
        m = GROUP * r + rel[k]
        return (pltpu.make_async_copy(mom_ref.at[m], fbuf.at[slot], f_sem.at[slot]),
                pltpu.make_async_copy(grad_ref.at[m], hbuf.at[slot], h_sem.at[slot]))

    def stage_m(r, k, slot):
        dst = xin.at[r, pl.ds(0, rows)] if k == 0 else mb.at[r, k - 1]
        return pltpu.make_async_copy(sbuf.at[slot], dst, st_sem.at[slot])

    def send_sum(r, k):
        return remote(ss_loc.at[r, k - 1], ss_in.at[r, k], s_send.at[r, k - 1], s_recv.at[r, k - 1], k)

    def send_m(r, k):
        return (remote(mb.at[r, k - 1], xin.at[r, pl.ds(k * rows, rows)], m_send.at[r, k - 1], m_recv.at[r, k - 1], k),
                send_sum(r, k))

    def block_m(r, j):
        k, slot = ORDER[j], j % 2
        for copy in load_m(r, k, slot):
            copy.wait()
        if j + 1 < GROUP:
            for copy in load_m(r, ORDER[j + 1], 1 - slot):
                copy.start()
        else:
            @pl.when(r + 1 < rounds)
            def _():
                for copy in load_m(r + 1, ORDER[0], 1 - slot):
                    copy.start()

        keep_sum(r, k, lax.fori_loop(0, rows // strip, momentum_strip(slot), jnp.zeros((8, cols), jnp.float32)))
        stage_m(r, k, slot).start()

    def momentum_strip(slot):
        def part(i, acc):
            sl = pl.ds(pl.multiple_of(i * strip, strip), strip)
            mom_new = MOMENTUM * fbuf[slot, sl, :] + hbuf[slot, sl, :].astype(jnp.float32)
            sbuf[slot, sl, :] = mom_new.astype(jnp.bfloat16)
            return acc + jnp.sum((mom_new * mom_new).reshape(strip // 8, 8, cols), axis=0)

        return part

    def keep_sum(r, k, acc):
        total = jnp.broadcast_to(jnp.sum(jnp.sum(acc, axis=0, keepdims=True), axis=1, keepdims=True), (8, 128))
        if k == 0:
            ss_in[r, 0] = total
        else:
            ss_loc[r, k - 1] = total

    def staged_m(r, j):
        stage_m(r, ORDER[j], j % 2).wait()
        if ORDER[j] != 0:
            for copy in send_m(r, ORDER[j]):
                copy.start()

    first, height = ORDER[0], rows // PIECES
    pieces = [pl.ds(n * height, height) for n in range(PIECES)]

    def load_piece(n):
        m = rel[first]
        return (pltpu.make_async_copy(mom_ref.at[m, pieces[n]], fbuf.at[0, pieces[n]], pf_sem.at[n]),
                pltpu.make_async_copy(grad_ref.at[m, pieces[n]], hbuf.at[0, pieces[n]], ph_sem.at[n]))

    def stage_piece(n):
        return pltpu.make_async_copy(sbuf.at[0, pieces[n]], mb.at[0, first - 1, pieces[n]], ps_sem.at[n])

    def send_piece(n):
        stage_piece(n).wait()
        remote(mb.at[0, first - 1, pieces[n]], xin.at[0, pl.ds(first * rows + n * height, height)],
               m_send.at[0, first - 1], m_recv.at[0, first - 1], first).start()

    for p in range(PIECES):
        for copy in load_piece(p):
            copy.start()
    for copy in load_m(0, ORDER[1], 1):
        copy.start()
    acc = jnp.zeros((8, cols), jnp.float32)
    for p in range(PIECES):
        for copy in load_piece(p):
            copy.wait()
        acc = lax.fori_loop(p * height // strip, (p + 1) * height // strip, momentum_strip(0), acc)
        stage_piece(p).start()
        if p == 0:
            pl.semaphore_wait(barrier, GROUP - 1)
        else:
            send_piece(p - 1)
    keep_sum(0, first, acc)
    send_piece(PIECES - 1)

    def momentum_round(r, carry):
        @pl.when(r > 0)
        def _():
            block_m(r, 0)
            staged_m(r - 1, GROUP - 1)

        block_m(r, 1)

        @pl.when(r > 0)
        def _():
            staged_m(r, 0)

        @pl.when(r == 0)
        def _():
            send_sum(r, first).start()

        for j in range(2, GROUP):
            block_m(r, j)
            staged_m(r, j - 1)
        return carry

    lax.fori_loop(0, rounds, momentum_round, 0)
    staged_m(rounds - 1, GROUP - 1)

    def send_o(r, k):
        return remote(oo.at[r, pl.ds(k * rows, rows)], orv.at[r, rel[0]], o_send.at[r, k - 1], o_recv.at[r, k - 1], k)

    def ortho_round(r, carry):
        for k in (1, 2, 3):
            for copy in send_m(r, k):
                copy.wait_recv()
        fetch = pltpu.make_async_copy(xin.at[r], xa, x_sem)
        fetch.start()
        fetch.wait()
        total = ss_in[r, 0] + ss_in[r, 1] + ss_in[r, 2] + ss_in[r, 3]
        denom = (jnp.sqrt(total) + NORM_EPS)[0:1, 0:1]

        def scale(i, c):
            sl = pl.ds(pl.multiple_of(i * strip, strip), strip)
            xb[sl, :] = (xa[sl, :].astype(jnp.float32) / denom).astype(jnp.bfloat16)
            return c

        lax.fori_loop(0, GROUP * rows // strip, scale, 0)

        def iterate(_, c):
            x_mat = xb[...]
            amat[...] = lax.dot_general(x_mat, x_mat, (((0,), (0,)), ((), ())),
                                        preferred_element_type=jnp.float32).astype(jnp.bfloat16)
            a_mat = amat[...]
            square = jnp.dot(a_mat, a_mat, preferred_element_type=jnp.float32)
            bmat[...] = (COEF_B * a_mat.astype(jnp.float32) + COEF_C * square).astype(jnp.bfloat16)

            def update(i, c2):
                sl = pl.ds(pl.multiple_of(i * rows, rows), rows)
                x_rows = xb[sl, :]
                prod = jnp.dot(x_rows, bmat[...], preferred_element_type=jnp.float32)
                xb[sl, :] = (COEF_A * x_rows.astype(jnp.float32) + prod).astype(jnp.bfloat16)
                return c2

            return lax.fori_loop(0, GROUP, update, c)

        lax.fori_loop(0, NS_ITERS, iterate, 0)
        kept = pltpu.make_async_copy(xb.at[pl.ds(0, rows)], orv.at[r, rel[0]], f_sem.at[0])
        out = pltpu.make_async_copy(xb, oo.at[r], x_sem)
        out.start()
        kept.start()
        out.wait()
        for k in ORDER[:3]:
            send_o(r, k).start()
        kept.wait()
        return carry

    lax.fori_loop(0, rounds, ortho_round, 0)

    def load_w(m, slot):
        return (pltpu.make_async_copy(w_ref.at[m], fbuf.at[slot], f_sem.at[slot]),
                pltpu.make_async_copy(orv.at[m // GROUP, lax.rem(m, GROUP)], hbuf.at[slot], h_sem.at[slot]))

    def load_round(m, slot):
        for k in (1, 2, 3):
            send_o(m // GROUP, k).wait_recv()
        for copy in load_w(m, slot):
            copy.start()

    def stage_w(c, i, slot):
        return pltpu.make_async_copy(sbuf.at[slot], w_outs[c].at[i], st_sem.at[slot])

    def send_w(i):
        return remote(w_outs[0].at[i], w_chip.at[i], w_send.at[i], w_recv.at[i], 2)

    mats = GROUP * rounds
    load_round(0, 0)

    def weights(m, carry):
        slot, later = lax.rem(m, 2), m + 1
        for copy in load_w(m, slot):
            copy.wait()

        @pl.when(lax.rem(later, GROUP) != 0)
        def _():
            for copy in load_w(later, 1 - slot):
                copy.start()

        @pl.when(m >= 2)
        def _():
            stage_w(0, 0, slot).wait()

        @pl.when((m == CHUNKS[0] + 1) & (lax.rem(rel[0], 2) == 0))
        def _():
            for i in range(CHUNKS[0]):
                send_w(i).start()

        def part(i, c):
            sl = pl.ds(pl.multiple_of(i * strip, strip), strip)
            w_old = fbuf[slot, sl, :]
            ortho = hbuf[slot, sl, :].astype(jnp.float32) * rms_scale
            sbuf[slot, sl, :] = (w_old - LEARN_RATE * (ortho + WEIGHT_DECAY * w_old)).astype(jnp.bfloat16)
            return c

        lax.fori_loop(0, rows // strip, part, 0)
        for c in range(len(CHUNKS)):
            @pl.when((m >= FIRSTS[c]) & (m < FIRSTS[c] + CHUNKS[c]))
            def _():
                stage_w(c, m - FIRSTS[c], slot).start()

        @pl.when((lax.rem(later, GROUP) == 0) & (later < mats))
        def _():
            load_round(later, 1 - slot)

        return carry

    lax.fori_loop(0, mats, weights, 0)
    stage_w(0, 0, 0).wait()
    stage_w(0, 0, 1).wait()

    @pl.when(lax.rem(rel[0], 2) == 0)
    def _():
        send_w(0).wait_send()
        pl.semaphore_signal(turn, inc=1, device_id={"data": rel[1]}, device_id_type=pl.DeviceIdType.MESH)
        for i in range(1, CHUNKS[0]):
            send_w(i).wait_send()

    @pl.when(lax.rem(rel[0], 2) == 1)
    def _():
        pl.semaphore_wait(turn, 1)
        for i in range(CHUNKS[0]):
            send_w(i).start()
        for i in range(CHUNKS[0]):
            send_w(i).wait_send()

    for i in range(CHUNKS[0]):
        send_w(i).wait_recv()

    def drain(r, carry):
        for k in (1, 2, 3):
            for copy in send_m(r, k):
                copy.wait_send()
            send_o(r, k).wait_send()
        return carry

    lax.fori_loop(0, rounds, drain, 0)


def exchange(w_rows, mom_rows, grad_rows):
    mats, rows, cols = mom_rows.shape
    rounds = mats // GROUP
    half, full = jnp.bfloat16, jnp.float32
    rms_scale = 0.2 * math.sqrt(max(rows * GROUP, cols))
    shapes = [jax.ShapeDtypeStruct((count, rows, cols), half) for count in CHUNKS + CHUNKS[:1]] + [
        jax.ShapeDtypeStruct((rounds, 3, rows, cols), half),
        jax.ShapeDtypeStruct((rounds, GROUP * rows, cols), half),
        jax.ShapeDtypeStruct((rounds, GROUP * rows, cols), half),
        jax.ShapeDtypeStruct((rounds, GROUP, rows, cols), half),
    ]
    dma = pltpu.SemaphoreType.DMA
    flops = rounds * NS_ITERS * 2 * cols * cols * (2 * rows * GROUP + cols)
    outs = pl.pallas_call(
        functools.partial(exchange_kernel, rounds, rms_scale),
        out_shape=shapes,
        in_specs=[pl.BlockSpec(memory_space=pltpu.HBM)] * 3,
        out_specs=[pl.BlockSpec(memory_space=pltpu.HBM)] * len(shapes),
        scratch_shapes=[
            pltpu.VMEM((2, rows, cols), full),
            pltpu.VMEM((2, rows, cols), half),
            pltpu.VMEM((2, rows, cols), half),
            pltpu.VMEM((rounds, 3, 8, 128), full),
            pltpu.VMEM((rounds, GROUP, 8, 128), full),
            pltpu.VMEM((GROUP * rows, cols), half),
            pltpu.VMEM((GROUP * rows, cols), half),
            pltpu.VMEM((cols, cols), half),
            pltpu.VMEM((cols, cols), half),
            dma((2,)), dma((2,)), dma((2,)), dma,
            *[dma((rounds, 3))] * 6, *[dma((CHUNKS[0],))] * 2, pltpu.SemaphoreType.REGULAR,
            *[dma((PIECES,))] * 3,
        ],
        compiler_params=pltpu.CompilerParams(collective_id=0, has_side_effects=True, vmem_limit_bytes=60 * 1024 * 1024),
        cost_estimate=pl.CostEstimate(flops=flops, bytes_accessed=12 * mats * rows * cols, transcendentals=0),
        name="exchange",
    )(w_rows, mom_rows, grad_rows)
    return outs[: len(CHUNKS)], outs[len(CHUNKS)]


def place_kernel(first, parts, *refs):
    blocks, (out_ref, buf, in_sem, out_sem) = refs[: len(parts)], refs[-4:]
    count, rows, _ = blocks[0].shape
    rel = relations(lax.axis_index("data"))

    def fetch(i, n, slot):
        return pltpu.make_async_copy(blocks[n].at[i], buf.at[slot, n], in_sem.at[slot, n])

    def put(i, n, slot):
        dst = out_ref.at[first + i, pl.ds(pl.multiple_of(rel[parts[n]] * rows, rows), rows)]
        return pltpu.make_async_copy(buf.at[slot, n], dst, out_sem.at[slot, n])

    for n in range(len(parts)):
        fetch(0, n, 0).start()

    def step(i, carry):
        slot = lax.rem(i, 2)
        for n in range(len(parts)):
            @pl.when(i >= 1)
            def _():
                put(i - 1, n, 1 - slot).wait()

            @pl.when(i + 1 < count)
            def _():
                fetch(i + 1, n, 1 - slot).start()

        for n in range(len(parts)):
            fetch(i, n, slot).wait()
            put(i, n, slot).start()
        return carry

    lax.fori_loop(0, count, step, 0)
    for n in range(len(parts)):
        put(count - 1, n, (count - 1) % 2).wait()


def place(chunk, blocks, dst, mats):
    parts = tuple(blocks)
    count, rows, cols = blocks[parts[0]].shape
    args, aliases = [blocks[k] for k in parts], {}
    if dst is not None:
        aliases = {len(args): 0}
        args.append(dst)
    size = len(parts) * count * rows * cols
    dma = pltpu.SemaphoreType.DMA
    return pl.pallas_call(
        functools.partial(place_kernel, FIRSTS[chunk], parts),
        out_shape=jax.ShapeDtypeStruct((mats, rows * GROUP, cols), jnp.bfloat16),
        in_specs=[pl.BlockSpec(memory_space=pltpu.HBM)] * len(args),
        out_specs=pl.BlockSpec(memory_space=pltpu.HBM),
        scratch_shapes=[pltpu.VMEM((2, len(parts), rows, cols), jnp.bfloat16), dma((2, len(parts))), dma((2, len(parts)))],
        input_output_aliases=aliases,
        compiler_params=pltpu.CompilerParams(vmem_limit_bytes=67_043_328),
        cost_estimate=pl.CostEstimate(flops=size, bytes_accessed=4 * size, transcendentals=0),
        name="place",
    )(*args)


def solution(mesh):
    row_spec = P("stage", "data", None)
    full_spec = P("stage", None, None)
    last = len(CHUNKS) - 1

    def local_step(w_rows, mom_rows, grad_rows):
        mats = mom_rows.shape[0]
        own, w_chip = exchange(w_rows, mom_rows, grad_rows)
        chip, core, diag = [w_chip], [], []
        for c in range(1, last + 1):
            chip.append(lax.ppermute(own[c], "data", X_PERM))
        for c in range(last + 1):
            core.append(lax.ppermute(own[c], "data", CORE_PERM))
            diag.append(lax.ppermute(chip[c], "data", CORE_PERM))
        mom_late, grad_late, _ = lax.optimization_barrier((mom_rows, grad_rows, own[0]))
        mom_new = MOMENTUM * mom_late + grad_late.astype(jnp.float32)
        params = None
        for c in range(last):
            params = place(c, {0: own[c], 1: core[c], 2: chip[c], 3: diag[c]}, params, mats)
        params = place(last, {0: own[last], 1: core[last]}, params, mats)
        params = place(last, {2: chip[last]}, params, mats)
        params = place(last, {3: diag[last]}, params, mats)
        return params, mom_new

    return jax.shard_map(local_step, mesh=mesh, in_specs=(row_spec, row_spec, row_spec), out_specs=(full_spec, row_spec), check_vma=False)
```

```python
import functools
import math

import jax
import jax.numpy as jnp
from jax import lax
from jax.experimental import pallas as pl
from jax.experimental.pallas import tpu as pltpu
from jax.sharding import PartitionSpec as P


NS_ITERS = 5
MOMENTUM = 0.95
LEARN_RATE = 0.02
WEIGHT_DECAY = 0.1
NORM_EPS = 1e-7
COEF_A = 3.4445
COEF_B = -4.7750
COEF_C = 2.0315

GROUP = 4
CHUNKS = (2, 6, 8, 8, 4, 2, 1, 1)
FIRSTS = tuple(sum(CHUNKS[:c]) for c in range(len(CHUNKS)))
PIECES = 8
ORDER = (2, 3, 1, 0)
X_PERM = ((0, 2), (1, 3), (2, 0), (3, 1))
CORE_PERM = ((0, 1), (1, 0), (2, 3), (3, 2))


def relations(me):
    partner = me + 1 - 2 * lax.rem(me, 2)
    return me, partner, lax.rem(me + 2, GROUP), lax.rem(partner + 2, GROUP)


def exchange_kernel(rounds, rms_scale, w_ref, mom_ref, grad_ref, *refs):
    n = len(CHUNKS)
    w_outs, (w_chip, mb, xin, oo, orv) = refs[:n], refs[n : n + 5]
    (fbuf, hbuf, sbuf, ss_loc, ss_in, xa, xb, amat, bmat, f_sem, h_sem, st_sem, x_sem,
     m_send, m_recv, s_send, s_recv, o_send, o_recv, w_send, w_recv, turn,
     pf_sem, ph_sem, ps_sem) = refs[n + 5 :]
    rows, cols = mom_ref.shape[1], mom_ref.shape[2]
    rel = relations(lax.axis_index("data"))
    strip = 64

    barrier = pltpu.get_barrier_semaphore()
    for k in (1, 2, 3):
        pl.semaphore_signal(barrier, inc=1, device_id={"data": rel[k]}, device_id_type=pl.DeviceIdType.MESH)

    def remote(src, dst, send, recv, k):
        return pltpu.make_async_remote_copy(
            src_ref=src, dst_ref=dst, send_sem=send, recv_sem=recv,
            device_id={"data": rel[k]}, device_id_type=pl.DeviceIdType.MESH)

    def load_m(r, k, slot):
        m = GROUP * r + rel[k]
        return (pltpu.make_async_copy(mom_ref.at[m], fbuf.at[slot], f_sem.at[slot]),
                pltpu.make_async_copy(grad_ref.at[m], hbuf.at[slot], h_sem.at[slot]))

    def stage_m(r, k, slot):
        dst = xin.at[r, pl.ds(0, rows)] if k == 0 else mb.at[r, k - 1]
        return pltpu.make_async_copy(sbuf.at[slot], dst, st_sem.at[slot])

    def send_sum(r, k):
        return remote(ss_loc.at[r, k - 1, pl.ds(0, 1)], ss_in.at[r, k, pl.ds(0, 1)], s_send.at[r, k - 1], s_recv.at[r, k - 1], k)

    def send_m(r, k):
        return (remote(mb.at[r, k - 1], xin.at[r, pl.ds(k * rows, rows)], m_send.at[r, k - 1], m_recv.at[r, k - 1], k),
                send_sum(r, k))

    def block_m(r, j):
        k, slot = ORDER[j], j % 2
        for copy in load_m(r, k, slot):
            copy.wait()
        if j + 1 < GROUP:
            for copy in load_m(r, ORDER[j + 1], 1 - slot):
                copy.start()
        else:
            @pl.when(r + 1 < rounds)
            def _():
                for copy in load_m(r + 1, ORDER[0], 1 - slot):
                    copy.start()

        keep_sum(r, k, lax.fori_loop(0, rows // strip, momentum_strip(slot), jnp.zeros((8, cols), jnp.float32)))
        stage_m(r, k, slot).start()

    def momentum_strip(slot):
        def part(i, acc):
            sl = pl.ds(pl.multiple_of(i * strip, strip), strip)
            mom_new = MOMENTUM * fbuf[slot, sl, :] + hbuf[slot, sl, :].astype(jnp.float32)
            sbuf[slot, sl, :] = mom_new.astype(jnp.bfloat16)
            return acc + jnp.sum((mom_new * mom_new).reshape(strip // 8, 8, cols), axis=0)

        return part

    def keep_sum(r, k, acc):
        total = jnp.broadcast_to(jnp.sum(jnp.sum(acc, axis=0, keepdims=True), axis=1, keepdims=True), (8, 128))
        if k == 0:
            ss_in[r, 0] = total
        else:
            ss_loc[r, k - 1] = total

    def staged_m(r, j):
        stage_m(r, ORDER[j], j % 2).wait()
        if ORDER[j] != 0:
            for copy in send_m(r, ORDER[j]):
                copy.start()

    first, height = ORDER[0], rows // PIECES
    pieces = [pl.ds(n * height, height) for n in range(PIECES)]

    def load_piece(n):
        m = rel[first]
        return (pltpu.make_async_copy(mom_ref.at[m, pieces[n]], fbuf.at[0, pieces[n]], pf_sem.at[n]),
                pltpu.make_async_copy(grad_ref.at[m, pieces[n]], hbuf.at[0, pieces[n]], ph_sem.at[n]))

    def stage_piece(n):
        return pltpu.make_async_copy(sbuf.at[0, pieces[n]], mb.at[0, first - 1, pieces[n]], ps_sem.at[n])

    def send_piece(n):
        stage_piece(n).wait()
        remote(mb.at[0, first - 1, pieces[n]], xin.at[0, pl.ds(first * rows + n * height, height)],
               m_send.at[0, first - 1], m_recv.at[0, first - 1], first).start()

    for p in range(PIECES):
        for copy in load_piece(p):
            copy.start()
    for copy in load_m(0, ORDER[1], 1):
        copy.start()
    acc = jnp.zeros((8, cols), jnp.float32)
    for p in range(PIECES):
        for copy in load_piece(p):
            copy.wait()
        acc = lax.fori_loop(p * height // strip, (p + 1) * height // strip, momentum_strip(0), acc)
        stage_piece(p).start()
        if p == 0:
            pl.semaphore_wait(barrier, GROUP - 1)
        else:
            send_piece(p - 1)
    keep_sum(0, first, acc)
    send_piece(PIECES - 1)

    def momentum_round(r, carry):
        @pl.when(r > 0)
        def _():
            block_m(r, 0)
            staged_m(r - 1, GROUP - 1)

        block_m(r, 1)

        @pl.when(r > 0)
        def _():
            staged_m(r, 0)

        @pl.when(r == 0)
        def _():
            send_sum(r, first).start()

        for j in range(2, GROUP):
            block_m(r, j)
            staged_m(r, j - 1)
        return carry

    lax.fori_loop(0, rounds, momentum_round, 0)
    staged_m(rounds - 1, GROUP - 1)

    def send_o(r, k):
        return remote(oo.at[r, pl.ds(k * rows, rows)], orv.at[r, rel[0]], o_send.at[r, k - 1], o_recv.at[r, k - 1], k)

    def ortho_round(r, carry):
        for k in (1, 2, 3):
            for copy in send_m(r, k):
                copy.wait_recv()
        fetch = pltpu.make_async_copy(xin.at[r], xa, x_sem)
        fetch.start()
        fetch.wait()
        total = sum(ss_in[r, k, 0:1, :] for k in range(1, GROUP)) + ss_in[r, 0, 0:1, :]
        denom = (jnp.sqrt(total) + NORM_EPS)[:, 0:1]

        def scale(i, c):
            sl = pl.ds(pl.multiple_of(i * strip, strip), strip)
            xb[sl, :] = (xa[sl, :].astype(jnp.float32) / denom).astype(jnp.bfloat16)
            return c

        lax.fori_loop(0, GROUP * rows // strip, scale, 0)

        def iterate(_, c):
            x_mat = xb[...]
            amat[...] = lax.dot_general(x_mat, x_mat, (((0,), (0,)), ((), ())),
                                        preferred_element_type=jnp.float32).astype(jnp.bfloat16)
            a_mat = amat[...]
            square = jnp.dot(a_mat, a_mat, preferred_element_type=jnp.float32)
            bmat[...] = (COEF_B * a_mat.astype(jnp.float32) + COEF_C * square).astype(jnp.bfloat16)

            def update(i, c2):
                sl = pl.ds(pl.multiple_of(i * rows, rows), rows)
                x_rows = xb[sl, :]
                prod = jnp.dot(x_rows, bmat[...], preferred_element_type=jnp.float32)
                xb[sl, :] = (COEF_A * x_rows.astype(jnp.float32) + prod).astype(jnp.bfloat16)
                return c2

            return lax.fori_loop(0, GROUP, update, c)

        lax.fori_loop(0, NS_ITERS, iterate, 0)
        kept = pltpu.make_async_copy(xb.at[pl.ds(0, rows)], orv.at[r, rel[0]], f_sem.at[0])
        out = pltpu.make_async_copy(xb, oo.at[r], x_sem)
        out.start()
        kept.start()
        out.wait()
        for k in ORDER[:3]:
            send_o(r, k).start()
        kept.wait()
        return carry

    lax.fori_loop(0, rounds, ortho_round, 0)

    def load_w(m, slot):
        return (pltpu.make_async_copy(w_ref.at[m], fbuf.at[slot], f_sem.at[slot]),
                pltpu.make_async_copy(orv.at[m // GROUP, lax.rem(m, GROUP)], hbuf.at[slot], h_sem.at[slot]))

    def load_round(m, slot):
        for k in (1, 2, 3):
            send_o(m // GROUP, k).wait_recv()
        for copy in load_w(m, slot):
            copy.start()

    def stage_w(c, i, slot):
        return pltpu.make_async_copy(sbuf.at[slot], w_outs[c].at[i], st_sem.at[slot])

    def send_w(i):
        return remote(w_outs[0].at[i], w_chip.at[i], w_send.at[i], w_recv.at[i], 2)

    mats = GROUP * rounds
    load_round(0, 0)

    def weights(m, carry):
        slot, later = lax.rem(m, 2), m + 1
        for copy in load_w(m, slot):
            copy.wait()

        @pl.when(lax.rem(later, GROUP) != 0)
        def _():
            for copy in load_w(later, 1 - slot):
                copy.start()

        @pl.when(m >= 2)
        def _():
            stage_w(0, 0, slot).wait()

        @pl.when((m == CHUNKS[0] + 1) & (lax.rem(rel[0], 2) == 0))
        def _():
            for i in range(CHUNKS[0]):
                send_w(i).start()

        def part(i, c):
            sl = pl.ds(pl.multiple_of(i * strip, strip), strip)
            w_old = fbuf[slot, sl, :]
            ortho = hbuf[slot, sl, :].astype(jnp.float32) * rms_scale
            sbuf[slot, sl, :] = (w_old - LEARN_RATE * (ortho + WEIGHT_DECAY * w_old)).astype(jnp.bfloat16)
            return c

        lax.fori_loop(0, rows // strip, part, 0)
        for c in range(len(CHUNKS)):
            @pl.when((m >= FIRSTS[c]) & (m < FIRSTS[c] + CHUNKS[c]))
            def _():
                stage_w(c, m - FIRSTS[c], slot).start()

        @pl.when((lax.rem(later, GROUP) == 0) & (later < mats))
        def _():
            load_round(later, 1 - slot)

        return carry

    lax.fori_loop(0, mats, weights, 0)
    stage_w(0, 0, 0).wait()
    stage_w(0, 0, 1).wait()

    @pl.when(lax.rem(rel[0], 2) == 0)
    def _():
        send_w(0).wait_send()
        pl.semaphore_signal(turn, inc=1, device_id={"data": rel[1]}, device_id_type=pl.DeviceIdType.MESH)
        for i in range(1, CHUNKS[0]):
            send_w(i).wait_send()

    @pl.when(lax.rem(rel[0], 2) == 1)
    def _():
        pl.semaphore_wait(turn, 1)
        for i in range(CHUNKS[0]):
            send_w(i).start()
        for i in range(CHUNKS[0]):
            send_w(i).wait_send()

    for i in range(CHUNKS[0]):
        send_w(i).wait_recv()

    def drain(r, carry):
        for k in (1, 2, 3):
            for copy in send_m(r, k):
                copy.wait_send()
            send_o(r, k).wait_send()
        return carry

    lax.fori_loop(0, rounds, drain, 0)


def exchange(w_rows, mom_rows, grad_rows):
    mats, rows, cols = mom_rows.shape
    rounds = mats // GROUP
    half, full = jnp.bfloat16, jnp.float32
    rms_scale = 0.2 * math.sqrt(max(rows * GROUP, cols))
    shapes = [jax.ShapeDtypeStruct((count, rows, cols), half) for count in CHUNKS + CHUNKS[:1]] + [
        jax.ShapeDtypeStruct((rounds, 3, rows, cols), half),
        jax.ShapeDtypeStruct((rounds, GROUP * rows, cols), half),
        jax.ShapeDtypeStruct((rounds, GROUP * rows, cols), half),
        jax.ShapeDtypeStruct((rounds, GROUP, rows, cols), half),
    ]
    dma = pltpu.SemaphoreType.DMA
    flops = rounds * NS_ITERS * 2 * cols * cols * (2 * rows * GROUP + cols)
    outs = pl.pallas_call(
        functools.partial(exchange_kernel, rounds, rms_scale),
        out_shape=shapes,
        in_specs=[pl.BlockSpec(memory_space=pltpu.HBM)] * 3,
        out_specs=[pl.BlockSpec(memory_space=pltpu.HBM)] * len(shapes),
        scratch_shapes=[
            pltpu.VMEM((2, rows, cols), full),
            pltpu.VMEM((2, rows, cols), half),
            pltpu.VMEM((2, rows, cols), half),
            pltpu.VMEM((rounds, 3, 8, 128), full),
            pltpu.VMEM((rounds, GROUP, 8, 128), full),
            pltpu.VMEM((GROUP * rows, cols), half),
            pltpu.VMEM((GROUP * rows, cols), half),
            pltpu.VMEM((cols, cols), half),
            pltpu.VMEM((cols, cols), half),
            dma((2,)), dma((2,)), dma((2,)), dma,
            *[dma((rounds, 3))] * 6, *[dma((CHUNKS[0],))] * 2, pltpu.SemaphoreType.REGULAR,
            *[dma((PIECES,))] * 3,
        ],
        compiler_params=pltpu.CompilerParams(collective_id=0, has_side_effects=True, vmem_limit_bytes=60 * 1024 * 1024),
        cost_estimate=pl.CostEstimate(flops=flops, bytes_accessed=12 * mats * rows * cols, transcendentals=0),
        name="exchange",
    )(w_rows, mom_rows, grad_rows)
    return outs[: len(CHUNKS)], outs[len(CHUNKS)]


def place_kernel(first, parts, *refs):
    blocks, (out_ref, buf, in_sem, out_sem) = refs[: len(parts)], refs[-4:]
    count, rows, _ = blocks[0].shape
    rel = relations(lax.axis_index("data"))

    def fetch(i, n, slot):
        return pltpu.make_async_copy(blocks[n].at[i], buf.at[slot, n], in_sem.at[slot, n])

    def put(i, n, slot):
        dst = out_ref.at[first + i, pl.ds(pl.multiple_of(rel[parts[n]] * rows, rows), rows)]
        return pltpu.make_async_copy(buf.at[slot, n], dst, out_sem.at[slot, n])

    for n in range(len(parts)):
        fetch(0, n, 0).start()

    def step(i, carry):
        slot = lax.rem(i, 2)
        for n in range(len(parts)):
            @pl.when(i >= 1)
            def _():
                put(i - 1, n, 1 - slot).wait()

            @pl.when(i + 1 < count)
            def _():
                fetch(i + 1, n, 1 - slot).start()

        for n in range(len(parts)):
            fetch(i, n, slot).wait()
            put(i, n, slot).start()
        return carry

    lax.fori_loop(0, count, step, 0)
    for n in range(len(parts)):
        put(count - 1, n, (count - 1) % 2).wait()


def place(chunk, blocks, dst, mats):
    parts = tuple(blocks)
    count, rows, cols = blocks[parts[0]].shape
    args, aliases = [blocks[k] for k in parts], {}
    if dst is not None:
        aliases = {len(args): 0}
        args.append(dst)
    size = len(parts) * count * rows * cols
    dma = pltpu.SemaphoreType.DMA
    return pl.pallas_call(
        functools.partial(place_kernel, FIRSTS[chunk], parts),
        out_shape=jax.ShapeDtypeStruct((mats, rows * GROUP, cols), jnp.bfloat16),
        in_specs=[pl.BlockSpec(memory_space=pltpu.HBM)] * len(args),
        out_specs=pl.BlockSpec(memory_space=pltpu.HBM),
        scratch_shapes=[pltpu.VMEM((2, len(parts), rows, cols), jnp.bfloat16), dma((2, len(parts))), dma((2, len(parts)))],
        input_output_aliases=aliases,
        compiler_params=pltpu.CompilerParams(vmem_limit_bytes=67_043_328),
        cost_estimate=pl.CostEstimate(flops=size, bytes_accessed=4 * size, transcendentals=0),
        name="place",
    )(*args)


def solution(mesh):
    row_spec = P("stage", "data", None)
    full_spec = P("stage", None, None)
    last = len(CHUNKS) - 1

    def local_step(w_rows, mom_rows, grad_rows):
        mats = mom_rows.shape[0]
        own, w_chip = exchange(w_rows, mom_rows, grad_rows)
        chip, core, diag = [w_chip], [], []
        for c in range(1, last + 1):
            chip.append(lax.ppermute(own[c], "data", X_PERM))
        for c in range(last + 1):
            core.append(lax.ppermute(own[c], "data", CORE_PERM))
            diag.append(lax.ppermute(chip[c], "data", CORE_PERM))
        mom_late, grad_late, _ = lax.optimization_barrier((mom_rows, grad_rows, own[0]))
        mom_new = MOMENTUM * mom_late + grad_late.astype(jnp.float32)
        params = None
        for c in range(last):
            params = place(c, {0: own[c], 1: core[c], 2: chip[c], 3: diag[c]}, params, mats)
        params = place(last, {0: own[last], 1: core[last]}, params, mats)
        params = place(last, {2: chip[last]}, params, mats)
        params = place(last, {3: diag[last]}, params, mats)
        return params, mom_new

    return jax.shard_map(local_step, mesh=mesh, in_specs=(row_spec, row_spec, row_spec), out_specs=(full_spec, row_spec), check_vma=False)
```

```python
import functools
import math

import jax
import jax.numpy as jnp
from jax import lax
from jax.experimental import pallas as pl
from jax.experimental.pallas import tpu as pltpu
from jax.sharding import PartitionSpec as P


NS_ITERS = 5
MOMENTUM = 0.95
LEARN_RATE = 0.02
WEIGHT_DECAY = 0.1
NORM_EPS = 1e-7
COEF_A = 3.4445
COEF_B = -4.7750
COEF_C = 2.0315

GROUP = 4
CHUNKS = (2, 6, 8, 8, 4, 2, 1, 1)
FIRSTS = tuple(sum(CHUNKS[:c]) for c in range(len(CHUNKS)))
PIECES = 8
ORDER = (2, 3, 1, 0)
X_PERM = ((0, 2), (1, 3), (2, 0), (3, 1))
CORE_PERM = ((0, 1), (1, 0), (2, 3), (3, 2))


def relations(me):
    partner = me + 1 - 2 * lax.rem(me, 2)
    return me, partner, lax.rem(me + 2, GROUP), lax.rem(partner + 2, GROUP)


def exchange_kernel(rounds, rms_scale, w_ref, mom_ref, grad_ref, *refs):
    n = len(CHUNKS)
    w_outs, (w_chip, mb, xin, oo, orv) = refs[:n], refs[n : n + 5]
    (fbuf, hbuf, sbuf, ss_loc, ss_in, xa, xb, amat, bmat, f_sem, h_sem, st_sem, x_sem,
     m_send, m_recv, s_send, s_recv, o_send, o_recv, w_send, w_recv, turn,
     pf_sem, ph_sem, ps_sem, vbuf) = refs[n + 5 :]
    rows, cols = mom_ref.shape[1], mom_ref.shape[2]
    rel = relations(lax.axis_index("data"))
    strip = 64

    barrier = pltpu.get_barrier_semaphore()
    for k in (1, 2, 3):
        pl.semaphore_signal(barrier, inc=1, device_id={"data": rel[k]}, device_id_type=pl.DeviceIdType.MESH)

    def remote(src, dst, send, recv, k):
        return pltpu.make_async_remote_copy(
            src_ref=src, dst_ref=dst, send_sem=send, recv_sem=recv,
            device_id={"data": rel[k]}, device_id_type=pl.DeviceIdType.MESH)

    def load_m(r, k, slot):
        m = GROUP * r + rel[k]
        return (pltpu.make_async_copy(mom_ref.at[m], fbuf.at[slot], f_sem.at[slot]),
                pltpu.make_async_copy(grad_ref.at[m], hbuf.at[slot], h_sem.at[slot]))

    def stage_m(r, k, slot):
        dst = xin.at[r, pl.ds(0, rows)] if k == 0 else mb.at[r, k - 1]
        return pltpu.make_async_copy(sbuf.at[slot], dst, st_sem.at[slot])

    def send_sum(r, k):
        return remote(ss_loc.at[r, k - 1, pl.ds(0, 1)], ss_in.at[r, k, pl.ds(0, 1)], s_send.at[r, k - 1], s_recv.at[r, k - 1], k)

    def send_m(r, k):
        return (remote(mb.at[r, k - 1], xin.at[r, pl.ds(k * rows, rows)], m_send.at[r, k - 1], m_recv.at[r, k - 1], k),
                send_sum(r, k))

    def block_m(r, j):
        k, slot = ORDER[j], j % 2
        for copy in load_m(r, k, slot):
            copy.wait()
        if j + 1 < GROUP:
            for copy in load_m(r, ORDER[j + 1], 1 - slot):
                copy.start()
        else:
            @pl.when(r + 1 < rounds)
            def _():
                for copy in load_m(r + 1, ORDER[0], 1 - slot):
                    copy.start()

        keep_sum(r, k, lax.fori_loop(0, rows // strip, momentum_strip(slot), jnp.zeros((8, cols), jnp.float32)))
        stage_m(r, k, slot).start()

    def momentum_strip(slot):
        def part(i, acc):
            sl = pl.ds(pl.multiple_of(i * strip, strip), strip)
            mom_new = MOMENTUM * fbuf[slot, sl, :] + hbuf[slot, sl, :].astype(jnp.float32)
            sbuf[slot, sl, :] = mom_new.astype(jnp.bfloat16)
            return acc + jnp.sum((mom_new * mom_new).reshape(strip // 8, 8, cols), axis=0)

        return part

    def keep_sum(r, k, acc):
        total = jnp.broadcast_to(jnp.sum(jnp.sum(acc, axis=0, keepdims=True), axis=1, keepdims=True), (8, 128))
        if k == 0:
            ss_in[r, 0] = total
        else:
            ss_loc[r, k - 1] = total

    def staged_m(r, j):
        stage_m(r, ORDER[j], j % 2).wait()
        if ORDER[j] != 0:
            for copy in send_m(r, ORDER[j]):
                copy.start()

    first, height = ORDER[0], rows // PIECES
    pieces = [pl.ds(n * height, height) for n in range(PIECES)]

    def load_piece(n):
        m = rel[first]
        return (pltpu.make_async_copy(mom_ref.at[m, pieces[n]], fbuf.at[0, pieces[n]], pf_sem.at[n]),
                pltpu.make_async_copy(grad_ref.at[m, pieces[n]], hbuf.at[0, pieces[n]], ph_sem.at[n]))

    def stage_piece(n):
        return pltpu.make_async_copy(sbuf.at[0, pieces[n]], vbuf.at[pieces[n]], ps_sem.at[n])

    def send_piece(n):
        stage_piece(n).wait()
        remote(vbuf.at[pieces[n]], xin.at[0, pl.ds(first * rows + n * height, height)],
               m_send.at[0, first - 1], m_recv.at[0, first - 1], first).start()

    for p in range(PIECES):
        for copy in load_piece(p):
            copy.start()
    for copy in load_m(0, ORDER[1], 1):
        copy.start()
    acc = jnp.zeros((8, cols), jnp.float32)
    for p in range(PIECES):
        for copy in load_piece(p):
            copy.wait()
        acc = lax.fori_loop(p * height // strip, (p + 1) * height // strip, momentum_strip(0), acc)
        stage_piece(p).start()
        if p == 0:
            pl.semaphore_wait(barrier, GROUP - 1)
        else:
            send_piece(p - 1)
    keep_sum(0, first, acc)
    send_piece(PIECES - 1)

    def momentum_round(r, carry):
        @pl.when(r > 0)
        def _():
            block_m(r, 0)
            staged_m(r - 1, GROUP - 1)

        block_m(r, 1)

        @pl.when(r > 0)
        def _():
            staged_m(r, 0)

        @pl.when(r == 0)
        def _():
            send_sum(r, first).start()

        for j in range(2, GROUP):
            block_m(r, j)
            staged_m(r, j - 1)
        return carry

    lax.fori_loop(0, rounds, momentum_round, 0)
    staged_m(rounds - 1, GROUP - 1)

    def send_o(r, k):
        return remote(oo.at[r, pl.ds(k * rows, rows)], orv.at[r, rel[0]], o_send.at[r, k - 1], o_recv.at[r, k - 1], k)

    def ortho_round(r, carry):
        for k in (1, 2, 3):
            for copy in send_m(r, k):
                copy.wait_recv()
        fetch = pltpu.make_async_copy(xin.at[r], xa, x_sem)
        fetch.start()
        fetch.wait()
        total = sum(ss_in[r, k, 0:1, :] for k in range(1, GROUP)) + ss_in[r, 0, 0:1, :]
        denom = (jnp.sqrt(total) + NORM_EPS)[:, 0:1]

        def scale(i, c):
            sl = pl.ds(pl.multiple_of(i * strip, strip), strip)
            xb[sl, :] = (xa[sl, :].astype(jnp.float32) / denom).astype(jnp.bfloat16)
            return c

        lax.fori_loop(0, GROUP * rows // strip, scale, 0)

        def iterate(_, c):
            x_mat = xb[...]
            amat[...] = lax.dot_general(x_mat, x_mat, (((0,), (0,)), ((), ())),
                                        preferred_element_type=jnp.float32).astype(jnp.bfloat16)
            a_mat = amat[...]
            square = jnp.dot(a_mat, a_mat, preferred_element_type=jnp.float32)
            bmat[...] = (COEF_B * a_mat.astype(jnp.float32) + COEF_C * square).astype(jnp.bfloat16)

            def update(i, c2):
                sl = pl.ds(pl.multiple_of(i * rows, rows), rows)
                x_rows = xb[sl, :]
                prod = jnp.dot(x_rows, bmat[...], preferred_element_type=jnp.float32)
                xb[sl, :] = (COEF_A * x_rows.astype(jnp.float32) + prod).astype(jnp.bfloat16)
                return c2

            return lax.fori_loop(0, GROUP, update, c)

        lax.fori_loop(0, NS_ITERS, iterate, 0)
        kept = pltpu.make_async_copy(xb.at[pl.ds(0, rows)], orv.at[r, rel[0]], f_sem.at[0])
        out = pltpu.make_async_copy(xb, oo.at[r], x_sem)
        out.start()
        kept.start()
        out.wait()
        for k in ORDER[:3]:
            send_o(r, k).start()
        kept.wait()
        return carry

    lax.fori_loop(0, rounds, ortho_round, 0)

    def load_w(m, slot):
        return (pltpu.make_async_copy(w_ref.at[m], fbuf.at[slot], f_sem.at[slot]),
                pltpu.make_async_copy(orv.at[m // GROUP, lax.rem(m, GROUP)], hbuf.at[slot], h_sem.at[slot]))

    def load_round(m, slot):
        for k in (1, 2, 3):
            send_o(m // GROUP, k).wait_recv()
        for copy in load_w(m, slot):
            copy.start()

    def stage_w(c, i, slot):
        return pltpu.make_async_copy(sbuf.at[slot], w_outs[c].at[i], st_sem.at[slot])

    def send_w(i):
        return remote(w_outs[0].at[i], w_chip.at[i], w_send.at[i], w_recv.at[i], 2)

    mats = GROUP * rounds
    load_round(0, 0)

    def weights(m, carry):
        slot, later = lax.rem(m, 2), m + 1
        for copy in load_w(m, slot):
            copy.wait()

        @pl.when(lax.rem(later, GROUP) != 0)
        def _():
            for copy in load_w(later, 1 - slot):
                copy.start()

        @pl.when(m >= 2)
        def _():
            stage_w(0, 0, slot).wait()

        @pl.when((m == CHUNKS[0] + 1) & (lax.rem(rel[0], 2) == 0))
        def _():
            for i in range(CHUNKS[0]):
                send_w(i).start()

        def part(i, c):
            sl = pl.ds(pl.multiple_of(i * strip, strip), strip)
            w_old = fbuf[slot, sl, :]
            ortho = hbuf[slot, sl, :].astype(jnp.float32) * rms_scale
            sbuf[slot, sl, :] = (w_old - LEARN_RATE * (ortho + WEIGHT_DECAY * w_old)).astype(jnp.bfloat16)
            return c

        lax.fori_loop(0, rows // strip, part, 0)
        for c in range(len(CHUNKS)):
            @pl.when((m >= FIRSTS[c]) & (m < FIRSTS[c] + CHUNKS[c]))
            def _():
                stage_w(c, m - FIRSTS[c], slot).start()

        @pl.when((lax.rem(later, GROUP) == 0) & (later < mats))
        def _():
            load_round(later, 1 - slot)

        return carry

    lax.fori_loop(0, mats, weights, 0)
    stage_w(0, 0, 0).wait()
    stage_w(0, 0, 1).wait()

    @pl.when(lax.rem(rel[0], 2) == 0)
    def _():
        send_w(0).wait_send()
        pl.semaphore_signal(turn, inc=1, device_id={"data": rel[1]}, device_id_type=pl.DeviceIdType.MESH)
        for i in range(1, CHUNKS[0]):
            send_w(i).wait_send()

    @pl.when(lax.rem(rel[0], 2) == 1)
    def _():
        pl.semaphore_wait(turn, 1)
        for i in range(CHUNKS[0]):
            send_w(i).start()
        for i in range(CHUNKS[0]):
            send_w(i).wait_send()

    for i in range(CHUNKS[0]):
        send_w(i).wait_recv()

    def drain(r, carry):
        for k in (1, 2, 3):
            for copy in send_m(r, k):
                copy.wait_send()
            send_o(r, k).wait_send()
        return carry

    lax.fori_loop(0, rounds, drain, 0)


def exchange(w_rows, mom_rows, grad_rows):
    mats, rows, cols = mom_rows.shape
    rounds = mats // GROUP
    half, full = jnp.bfloat16, jnp.float32
    rms_scale = 0.2 * math.sqrt(max(rows * GROUP, cols))
    shapes = [jax.ShapeDtypeStruct((count, rows, cols), half) for count in CHUNKS + CHUNKS[:1]] + [
        jax.ShapeDtypeStruct((rounds, 3, rows, cols), half),
        jax.ShapeDtypeStruct((rounds, GROUP * rows, cols), half),
        jax.ShapeDtypeStruct((rounds, GROUP * rows, cols), half),
        jax.ShapeDtypeStruct((rounds, GROUP, rows, cols), half),
    ]
    dma = pltpu.SemaphoreType.DMA
    flops = rounds * NS_ITERS * 2 * cols * cols * (2 * rows * GROUP + cols)
    outs = pl.pallas_call(
        functools.partial(exchange_kernel, rounds, rms_scale),
        out_shape=shapes,
        in_specs=[pl.BlockSpec(memory_space=pltpu.HBM)] * 3,
        out_specs=[pl.BlockSpec(memory_space=pltpu.HBM)] * len(shapes),
        scratch_shapes=[
            pltpu.VMEM((2, rows, cols), full),
            pltpu.VMEM((2, rows, cols), half),
            pltpu.VMEM((2, rows, cols), half),
            pltpu.VMEM((rounds, 3, 8, 128), full),
            pltpu.VMEM((rounds, GROUP, 8, 128), full),
            pltpu.VMEM((GROUP * rows, cols), half),
            pltpu.VMEM((GROUP * rows, cols), half),
            pltpu.VMEM((cols, cols), half),
            pltpu.VMEM((cols, cols), half),
            dma((2,)), dma((2,)), dma((2,)), dma,
            *[dma((rounds, 3))] * 6, *[dma((CHUNKS[0],))] * 2, pltpu.SemaphoreType.REGULAR,
            *[dma((PIECES,))] * 3,
            pltpu.VMEM((rows, cols), half),
        ],
        compiler_params=pltpu.CompilerParams(collective_id=0, has_side_effects=True, vmem_limit_bytes=60 * 1024 * 1024),
        cost_estimate=pl.CostEstimate(flops=flops, bytes_accessed=12 * mats * rows * cols, transcendentals=0),
        name="exchange",
    )(w_rows, mom_rows, grad_rows)
    return outs[: len(CHUNKS)], outs[len(CHUNKS)]


def place_kernel(first, parts, *refs):
    blocks, (out_ref, buf, in_sem, out_sem) = refs[: len(parts)], refs[-4:]
    count, rows, _ = blocks[0].shape
    rel = relations(lax.axis_index("data"))

    def fetch(i, n, slot):
        return pltpu.make_async_copy(blocks[n].at[i], buf.at[slot, n], in_sem.at[slot, n])

    def put(i, n, slot):
        dst = out_ref.at[first + i, pl.ds(pl.multiple_of(rel[parts[n]] * rows, rows), rows)]
        return pltpu.make_async_copy(buf.at[slot, n], dst, out_sem.at[slot, n])

    for n in range(len(parts)):
        fetch(0, n, 0).start()

    def step(i, carry):
        slot = lax.rem(i, 2)
        for n in range(len(parts)):
            @pl.when(i >= 1)
            def _():
                put(i - 1, n, 1 - slot).wait()

            @pl.when(i + 1 < count)
            def _():
                fetch(i + 1, n, 1 - slot).start()

        for n in range(len(parts)):
            fetch(i, n, slot).wait()
            put(i, n, slot).start()
        return carry

    lax.fori_loop(0, count, step, 0)
    for n in range(len(parts)):
        put(count - 1, n, (count - 1) % 2).wait()


def place(chunk, blocks, dst, mats):
    parts = tuple(blocks)
    count, rows, cols = blocks[parts[0]].shape
    args, aliases = [blocks[k] for k in parts], {}
    if dst is not None:
        aliases = {len(args): 0}
        args.append(dst)
    size = len(parts) * count * rows * cols
    dma = pltpu.SemaphoreType.DMA
    return pl.pallas_call(
        functools.partial(place_kernel, FIRSTS[chunk], parts),
        out_shape=jax.ShapeDtypeStruct((mats, rows * GROUP, cols), jnp.bfloat16),
        in_specs=[pl.BlockSpec(memory_space=pltpu.HBM)] * len(args),
        out_specs=pl.BlockSpec(memory_space=pltpu.HBM),
        scratch_shapes=[pltpu.VMEM((2, len(parts), rows, cols), jnp.bfloat16), dma((2, len(parts))), dma((2, len(parts)))],
        input_output_aliases=aliases,
        compiler_params=pltpu.CompilerParams(vmem_limit_bytes=67_043_328),
        cost_estimate=pl.CostEstimate(flops=size, bytes_accessed=4 * size, transcendentals=0),
        name="place",
    )(*args)


def solution(mesh):
    row_spec = P("stage", "data", None)
    full_spec = P("stage", None, None)
    last = len(CHUNKS) - 1

    def local_step(w_rows, mom_rows, grad_rows):
        mats = mom_rows.shape[0]
        own, w_chip = exchange(w_rows, mom_rows, grad_rows)
        chip, core, diag = [w_chip], [], []
        for c in range(1, last + 1):
            chip.append(lax.ppermute(own[c], "data", X_PERM))
        for c in range(last + 1):
            core.append(lax.ppermute(own[c], "data", CORE_PERM))
            diag.append(lax.ppermute(chip[c], "data", CORE_PERM))
        mom_late, grad_late, _ = lax.optimization_barrier((mom_rows, grad_rows, own[0]))
        mom_new = MOMENTUM * mom_late + grad_late.astype(jnp.float32)
        params = None
        for c in range(last):
            params = place(c, {0: own[c], 1: core[c], 2: chip[c], 3: diag[c]}, params, mats)
        params = place(last, {0: own[last], 1: core[last]}, params, mats)
        params = place(last, {2: chip[last]}, params, mats)
        params = place(last, {3: diag[last]}, params, mats)
        return params, mom_new

    return jax.shard_map(local_step, mesh=mesh, in_specs=(row_spec, row_spec, row_spec), out_specs=(full_spec, row_spec), check_vma=False)
```

```python
import functools
import math

import jax
import jax.numpy as jnp
from jax import lax
from jax.experimental import pallas as pl
from jax.experimental.pallas import tpu as pltpu
from jax.sharding import PartitionSpec as P


NS_ITERS = 5
MOMENTUM = 0.95
LEARN_RATE = 0.02
WEIGHT_DECAY = 0.1
NORM_EPS = 1e-7
COEF_A = 3.4445
COEF_B = -4.7750
COEF_C = 2.0315

GROUP = 4
CHUNKS = (2, 6, 8, 8, 4, 2, 1, 1)
FIRSTS = tuple(sum(CHUNKS[:c]) for c in range(len(CHUNKS)))
PIECES = 8
ORDER = (2, 3, 1, 0)
X_PERM = ((0, 2), (1, 3), (2, 0), (3, 1))
CORE_PERM = ((0, 1), (1, 0), (2, 3), (3, 2))


def relations(me):
    partner = me + 1 - 2 * lax.rem(me, 2)
    return me, partner, lax.rem(me + 2, GROUP), lax.rem(partner + 2, GROUP)


def exchange_kernel(rounds, rms_scale, w_ref, mom_ref, grad_ref, *refs):
    n = len(CHUNKS) + 1
    w_outs, (w_chip, mb, xin, oo, orv) = refs[:n], refs[n : n + 5]
    (fbuf, hbuf, sbuf, ss_loc, ss_in, xa, xb, amat, bmat, f_sem, h_sem, st_sem, x_sem,
     m_send, m_recv, s_send, s_recv, o_send, o_recv, w_send, w_recv, turn,
     pf_sem, ph_sem, ps_sem, vbuf) = refs[n + 5 :]
    rows, cols = mom_ref.shape[1], mom_ref.shape[2]
    rel = relations(lax.axis_index("data"))
    strip = 64

    barrier = pltpu.get_barrier_semaphore()
    for k in (1, 2, 3):
        pl.semaphore_signal(barrier, inc=1, device_id={"data": rel[k]}, device_id_type=pl.DeviceIdType.MESH)

    def remote(src, dst, send, recv, k):
        return pltpu.make_async_remote_copy(
            src_ref=src, dst_ref=dst, send_sem=send, recv_sem=recv,
            device_id={"data": rel[k]}, device_id_type=pl.DeviceIdType.MESH)

    def load_m(r, k, slot):
        m = GROUP * r + rel[k]
        return (pltpu.make_async_copy(mom_ref.at[m], fbuf.at[slot], f_sem.at[slot]),
                pltpu.make_async_copy(grad_ref.at[m], hbuf.at[slot], h_sem.at[slot]))

    def stage_m(r, k, slot):
        dst = xin.at[r, pl.ds(0, rows)] if k == 0 else mb.at[r, k - 1]
        return pltpu.make_async_copy(sbuf.at[slot], dst, st_sem.at[slot])

    def send_sum(r, k):
        return remote(ss_loc.at[r, k - 1, pl.ds(0, 1)], ss_in.at[r, k, pl.ds(0, 1)], s_send.at[r, k - 1], s_recv.at[r, k - 1], k)

    def send_m(r, k):
        return (remote(mb.at[r, k - 1], xin.at[r, pl.ds(k * rows, rows)], m_send.at[r, k - 1], m_recv.at[r, k - 1], k),
                send_sum(r, k))

    def block_m(r, j):
        k, slot = ORDER[j], j % 2
        for copy in load_m(r, k, slot):
            copy.wait()
        if j + 1 < GROUP:
            for copy in load_m(r, ORDER[j + 1], 1 - slot):
                copy.start()
        else:
            @pl.when(r + 1 < rounds)
            def _():
                for copy in load_m(r + 1, ORDER[0], 1 - slot):
                    copy.start()

        keep_sum(r, k, lax.fori_loop(0, rows // strip, momentum_strip(slot), jnp.zeros((8, cols), jnp.float32)))
        stage_m(r, k, slot).start()

    def momentum_strip(slot):
        def part(i, acc):
            sl = pl.ds(pl.multiple_of(i * strip, strip), strip)
            mom_new = MOMENTUM * fbuf[slot, sl, :] + hbuf[slot, sl, :].astype(jnp.float32)
            sbuf[slot, sl, :] = mom_new.astype(jnp.bfloat16)
            return acc + jnp.sum((mom_new * mom_new).reshape(strip // 8, 8, cols), axis=0)

        return part

    def keep_sum(r, k, acc):
        total = jnp.broadcast_to(jnp.sum(jnp.sum(acc, axis=0, keepdims=True), axis=1, keepdims=True), (8, 128))
        if k == 0:
            ss_in[r, 0] = total
        else:
            ss_loc[r, k - 1] = total

    def staged_m(r, j):
        stage_m(r, ORDER[j], j % 2).wait()
        if ORDER[j] != 0:
            for copy in send_m(r, ORDER[j]):
                copy.start()

    first, height = ORDER[0], rows // PIECES
    pieces = [pl.ds(n * height, height) for n in range(PIECES)]

    def load_piece(n):
        m = rel[first]
        return (pltpu.make_async_copy(mom_ref.at[m, pieces[n]], fbuf.at[0, pieces[n]], pf_sem.at[n]),
                pltpu.make_async_copy(grad_ref.at[m, pieces[n]], hbuf.at[0, pieces[n]], ph_sem.at[n]))

    def stage_piece(n):
        return pltpu.make_async_copy(sbuf.at[0, pieces[n]], vbuf.at[pieces[n]], ps_sem.at[n])

    def send_piece(n):
        stage_piece(n).wait()
        remote(vbuf.at[pieces[n]], xin.at[0, pl.ds(first * rows + n * height, height)],
               m_send.at[0, first - 1], m_recv.at[0, first - 1], first).start()

    for p in range(PIECES):
        for copy in load_piece(p):
            copy.start()
    for copy in load_m(0, ORDER[1], 1):
        copy.start()
    acc = jnp.zeros((8, cols), jnp.float32)
    for p in range(PIECES):
        for copy in load_piece(p):
            copy.wait()
        acc = lax.fori_loop(p * height // strip, (p + 1) * height // strip, momentum_strip(0), acc)
        stage_piece(p).start()
        if p == 0:
            pl.semaphore_wait(barrier, GROUP - 1)
        else:
            send_piece(p - 1)
    keep_sum(0, first, acc)
    send_piece(PIECES - 1)

    def momentum_round(r, carry):
        @pl.when(r > 0)
        def _():
            block_m(r, 0)
            staged_m(r - 1, GROUP - 1)

        block_m(r, 1)

        @pl.when(r > 0)
        def _():
            staged_m(r, 0)

        @pl.when(r == 0)
        def _():
            send_sum(r, first).start()

        for j in range(2, GROUP):
            block_m(r, j)
            staged_m(r, j - 1)
        return carry

    lax.fori_loop(0, rounds, momentum_round, 0)
    staged_m(rounds - 1, GROUP - 1)

    def send_o(r, k):
        return remote(oo.at[r, pl.ds(k * rows, rows)], orv.at[r, rel[0]], o_send.at[r, k - 1], o_recv.at[r, k - 1], k)

    def ortho_round(r, carry):
        for k in (1, 2, 3):
            for copy in send_m(r, k):
                copy.wait_recv()
        fetch = pltpu.make_async_copy(xin.at[r], xa, x_sem)
        fetch.start()
        fetch.wait()
        total = sum(ss_in[r, k, 0:1, :] for k in range(1, GROUP)) + ss_in[r, 0, 0:1, :]
        denom = (jnp.sqrt(total) + NORM_EPS)[:, 0:1]

        def scale(i, c):
            sl = pl.ds(pl.multiple_of(i * strip, strip), strip)
            xb[sl, :] = (xa[sl, :].astype(jnp.float32) / denom).astype(jnp.bfloat16)
            return c

        lax.fori_loop(0, GROUP * rows // strip, scale, 0)

        def iterate(_, c):
            x_mat = xb[...]
            amat[...] = lax.dot_general(x_mat, x_mat, (((0,), (0,)), ((), ())),
                                        preferred_element_type=jnp.float32).astype(jnp.bfloat16)
            a_mat = amat[...]
            square = jnp.dot(a_mat, a_mat, preferred_element_type=jnp.float32)
            bmat[...] = (COEF_B * a_mat.astype(jnp.float32) + COEF_C * square).astype(jnp.bfloat16)

            def update(i, c2):
                sl = pl.ds(pl.multiple_of(i * rows, rows), rows)
                x_rows = xb[sl, :]
                prod = jnp.dot(x_rows, bmat[...], preferred_element_type=jnp.float32)
                xb[sl, :] = (COEF_A * x_rows.astype(jnp.float32) + prod).astype(jnp.bfloat16)
                return c2

            return lax.fori_loop(0, GROUP, update, c)

        lax.fori_loop(0, NS_ITERS, iterate, 0)
        kept = pltpu.make_async_copy(xb.at[pl.ds(0, rows)], orv.at[r, rel[0]], f_sem.at[0])
        out = pltpu.make_async_copy(xb, oo.at[r], x_sem)
        out.start()
        kept.start()
        out.wait()
        for k in ORDER[:3]:
            send_o(r, k).start()
        kept.wait()
        return carry

    lax.fori_loop(0, rounds, ortho_round, 0)

    def load_w(m, slot):
        return (pltpu.make_async_copy(w_ref.at[m], fbuf.at[slot], f_sem.at[slot]),
                pltpu.make_async_copy(orv.at[m // GROUP, lax.rem(m, GROUP)], hbuf.at[slot], h_sem.at[slot]))

    def load_round(m, slot):
        for k in (1, 2, 3):
            send_o(m // GROUP, k).wait_recv()
        for copy in load_w(m, slot):
            copy.start()

    def stage_w(c, i, slot):
        return pltpu.make_async_copy(sbuf.at[slot], w_outs[c].at[i], st_sem.at[slot])

    def send_w(i):
        return remote(w_outs[0].at[i], w_chip.at[i], w_send.at[i], w_recv.at[i], 2)

    mats = GROUP * rounds
    load_round(0, 0)

    def weights(m, carry):
        slot, later = lax.rem(m, 2), m + 1
        for copy in load_w(m, slot):
            copy.wait()

        @pl.when(lax.rem(later, GROUP) != 0)
        def _():
            for copy in load_w(later, 1 - slot):
                copy.start()

        @pl.when(m >= 2)
        def _():
            stage_w(0, 0, slot).wait()

        @pl.when((m == CHUNKS[0] + 1) & (lax.rem(rel[0], 2) == 0))
        def _():
            for i in range(CHUNKS[0]):
                send_w(i).start()

        def part(i, c):
            sl = pl.ds(pl.multiple_of(i * strip, strip), strip)
            w_old = fbuf[slot, sl, :]
            ortho = hbuf[slot, sl, :].astype(jnp.float32) * rms_scale
            sbuf[slot, sl, :] = (w_old - LEARN_RATE * (ortho + WEIGHT_DECAY * w_old)).astype(jnp.bfloat16)
            return c

        lax.fori_loop(0, rows // strip, part, 0)
        for c in range(len(CHUNKS)):
            @pl.when((m >= FIRSTS[c]) & (m < FIRSTS[c] + CHUNKS[c]))
            def _():
                if c + 1 < len(CHUNKS):
                    stage_w(c, m - FIRSTS[c], slot).start()
                else:
                    for h in range(2):
                        part_rows = sbuf.at[slot, pl.ds(h * rows // 2, rows // 2)]
                        pltpu.make_async_copy(part_rows, w_outs[c + h].at[0], st_sem.at[slot]).start()

        @pl.when((lax.rem(later, GROUP) == 0) & (later < mats))
        def _():
            load_round(later, 1 - slot)

        return carry

    lax.fori_loop(0, mats, weights, 0)
    stage_w(0, 0, 0).wait()
    stage_w(0, 0, 1).wait()

    @pl.when(lax.rem(rel[0], 2) == 0)
    def _():
        send_w(0).wait_send()
        pl.semaphore_signal(turn, inc=1, device_id={"data": rel[1]}, device_id_type=pl.DeviceIdType.MESH)
        for i in range(1, CHUNKS[0]):
            send_w(i).wait_send()

    @pl.when(lax.rem(rel[0], 2) == 1)
    def _():
        pl.semaphore_wait(turn, 1)
        for i in range(CHUNKS[0]):
            send_w(i).start()
        for i in range(CHUNKS[0]):
            send_w(i).wait_send()

    for i in range(CHUNKS[0]):
        send_w(i).wait_recv()

    def drain(r, carry):
        for k in (1, 2, 3):
            for copy in send_m(r, k):
                copy.wait_send()
            send_o(r, k).wait_send()
        return carry

    lax.fori_loop(0, rounds, drain, 0)


def exchange(w_rows, mom_rows, grad_rows):
    mats, rows, cols = mom_rows.shape
    rounds = mats // GROUP
    half, full = jnp.bfloat16, jnp.float32
    rms_scale = 0.2 * math.sqrt(max(rows * GROUP, cols))
    shapes = [jax.ShapeDtypeStruct((count, rows, cols), half) for count in CHUNKS[:-1]] + [
        jax.ShapeDtypeStruct((1, rows // 2, cols), half)] * 2 + [jax.ShapeDtypeStruct((CHUNKS[0], rows, cols), half)] + [
        jax.ShapeDtypeStruct((rounds, 3, rows, cols), half),
        jax.ShapeDtypeStruct((rounds, GROUP * rows, cols), half),
        jax.ShapeDtypeStruct((rounds, GROUP * rows, cols), half),
        jax.ShapeDtypeStruct((rounds, GROUP, rows, cols), half),
    ]
    dma = pltpu.SemaphoreType.DMA
    flops = rounds * NS_ITERS * 2 * cols * cols * (2 * rows * GROUP + cols)
    outs = pl.pallas_call(
        functools.partial(exchange_kernel, rounds, rms_scale),
        out_shape=shapes,
        in_specs=[pl.BlockSpec(memory_space=pltpu.HBM)] * 3,
        out_specs=[pl.BlockSpec(memory_space=pltpu.HBM)] * len(shapes),
        scratch_shapes=[
            pltpu.VMEM((2, rows, cols), full),
            pltpu.VMEM((2, rows, cols), half),
            pltpu.VMEM((2, rows, cols), half),
            pltpu.VMEM((rounds, 3, 8, 128), full),
            pltpu.VMEM((rounds, GROUP, 8, 128), full),
            pltpu.VMEM((GROUP * rows, cols), half),
            pltpu.VMEM((GROUP * rows, cols), half),
            pltpu.VMEM((cols, cols), half),
            pltpu.VMEM((cols, cols), half),
            dma((2,)), dma((2,)), dma((2,)), dma,
            *[dma((rounds, 3))] * 6, *[dma((CHUNKS[0],))] * 2, pltpu.SemaphoreType.REGULAR,
            *[dma((PIECES,))] * 3,
            pltpu.VMEM((rows, cols), half),
        ],
        compiler_params=pltpu.CompilerParams(collective_id=0, has_side_effects=True, vmem_limit_bytes=60 * 1024 * 1024),
        cost_estimate=pl.CostEstimate(flops=flops, bytes_accessed=12 * mats * rows * cols, transcendentals=0),
        name="exchange",
    )(w_rows, mom_rows, grad_rows)
    return outs[: len(CHUNKS) + 1], outs[len(CHUNKS) + 1]


def place_kernel(first, parts, height, offset, *refs):
    blocks, (out_ref, buf, in_sem, out_sem) = refs[: len(parts)], refs[-4:]
    count, rows, _ = blocks[0].shape
    rel = relations(lax.axis_index("data"))

    def fetch(i, n, slot):
        return pltpu.make_async_copy(blocks[n].at[i], buf.at[slot, n], in_sem.at[slot, n])

    def put(i, n, slot):
        dst = out_ref.at[first + i, pl.ds(pl.multiple_of(rel[parts[n]] * height + offset, rows), rows)]
        return pltpu.make_async_copy(buf.at[slot, n], dst, out_sem.at[slot, n])

    for n in range(len(parts)):
        fetch(0, n, 0).start()

    def step(i, carry):
        slot = lax.rem(i, 2)
        for n in range(len(parts)):
            @pl.when(i >= 1)
            def _():
                put(i - 1, n, 1 - slot).wait()

            @pl.when(i + 1 < count)
            def _():
                fetch(i + 1, n, 1 - slot).start()

        for n in range(len(parts)):
            fetch(i, n, slot).wait()
            put(i, n, slot).start()
        return carry

    lax.fori_loop(0, count, step, 0)
    for n in range(len(parts)):
        put(count - 1, n, (count - 1) % 2).wait()


def place(first, blocks, dst, mats, height, offset=0):
    parts = tuple(blocks)
    count, rows, cols = blocks[parts[0]].shape
    args, aliases = [blocks[k] for k in parts], {}
    if dst is not None:
        aliases = {len(args): 0}
        args.append(dst)
    size = len(parts) * count * rows * cols
    dma = pltpu.SemaphoreType.DMA
    return pl.pallas_call(
        functools.partial(place_kernel, first, parts, height, offset),
        out_shape=jax.ShapeDtypeStruct((mats, height * GROUP, cols), jnp.bfloat16),
        in_specs=[pl.BlockSpec(memory_space=pltpu.HBM)] * len(args),
        out_specs=pl.BlockSpec(memory_space=pltpu.HBM),
        scratch_shapes=[pltpu.VMEM((2, len(parts), rows, cols), jnp.bfloat16), dma((2, len(parts))), dma((2, len(parts)))],
        input_output_aliases=aliases,
        compiler_params=pltpu.CompilerParams(vmem_limit_bytes=67_043_328),
        cost_estimate=pl.CostEstimate(flops=size, bytes_accessed=4 * size, transcendentals=0),
        name="place",
    )(*args)


def solution(mesh):
    row_spec = P("stage", "data", None)
    full_spec = P("stage", None, None)
    last = len(CHUNKS)

    def local_step(w_rows, mom_rows, grad_rows):
        mats, height, _ = mom_rows.shape
        own, w_chip = exchange(w_rows, mom_rows, grad_rows)
        chip, core, diag = [w_chip], [], []
        for c in range(1, last + 1):
            chip.append(lax.ppermute(own[c], "data", X_PERM))
        for c in range(last + 1):
            core.append(lax.ppermute(own[c], "data", CORE_PERM))
            diag.append(lax.ppermute(chip[c], "data", CORE_PERM))
        mom_late, grad_late, _ = lax.optimization_barrier((mom_rows, grad_rows, own[0]))
        mom_new = MOMENTUM * mom_late + grad_late.astype(jnp.float32)
        params = None

        def whole(c):
            return {0: own[c], 1: core[c], 2: chip[c], 3: diag[c]}

        for c in range(last - 1):
            params = place(FIRSTS[c], whole(c), params, mats, height)
        params = place(mats - 1, {0: own[last], 1: core[last]}, params, mats, height, height // 2)
        params = place(mats - 1, whole(last - 1), params, mats, height)
        params = place(mats - 1, {2: chip[last]}, params, mats, height, height // 2)
        params = place(mats - 1, {3: diag[last]}, params, mats, height, height // 2)
        return params, mom_new

    return jax.shard_map(local_step, mesh=mesh, in_specs=(row_spec, row_spec, row_spec), out_specs=(full_spec, row_spec), check_vma=False)
```
